32 devices in a mesh: node: 4 (over y, core), local: 8 (over z, x).
Axes of the slice: x: 2, y: 2, z: 4, core: 2. Of those that a mesh axis runs over, the one named last changes fastest.
Arguments:
- tokens: bfloat16 [2048, 7168], P(('node', 'local')), may hold values from -6 to 6
- routes: int32 [2048, 8], P(('node', 'local')), may hold values from 0 to 15, as said below
- gates: bfloat16 [2048, 8], P(('node', 'local')), may hold values from 0.049804688 to 0.5
- w_in: bfloat16 [32, 3584, 2048], P(('node', 'local')), may hold values from -0.0625 to 0.0625
- w_out: bfloat16 [32, 1024, 3584], P(('node', 'local')), may hold values from -0.1875 to 0.1875
Outputs:
- combined: bfloat16 [2048, 7168], P(('node', 'local'))
The draws below stay inside these ranges and needn't reach their ends.
Inputs may be any that keep to these rules, and one draw needn't show every extreme that they name: `routes`: expert e belongs to node group e // 4. Each row names 8 different experts, 4 in each of exactly 2 node groups. Among the 64 rows of one device no expert is named more than 40 times, and some expert is named exactly 40 times by the rows of every device.
All inputs are finite; a program needn't handle non-finite values.
Results may differ from the reference program's by a relative error of at most 0.011.
Values may be sent and summed in bfloat16 or wider, within the bound.
A program may use at most 128 MiB of HBM per device.

```python
import math
import jax
import jax.numpy as jnp
from jax import lax

D = 7168
H = 1024
TOP = 8
TOK_DEV = 64
EXPERTS = 16
NODE_PICK = 2
SPECIALIST_CAP = 40
TOKENS = 2048
N_NODE = 4


def draw_routes(key, part):
    blocks = TOKENS // TOK_DEV
    per_node = EXPERTS // N_NODE
    take = TOP // NODE_PICK
    key_pop, key_hot, key_noise = jax.random.split(jax.random.fold_in(key, 11), 3)
    popular_specialists = jax.random.randint(key_pop, (EXPERTS,), 0, 4).astype(jnp.int32)
    preferred_specialist = jax.random.randint(key_hot, (), 0, EXPERTS).astype(jnp.int32)
    noise = jax.random.randint(key_noise, (blocks, TOK_DEV, EXPERTS), 0, 1024).astype(jnp.int32)
    specialist_numbers = jnp.arange(EXPERTS, dtype=jnp.int32)
    node_ids = jnp.arange(N_NODE, dtype=jnp.int32)

    def one_block(noise_block):

        def step(counts, random_perturbation):
            remaining_headroom = (SPECIALIST_CAP - counts).astype(jnp.int32)
            preferred_increment = 2048 * (SPECIALIST_CAP + 2) * (specialist_numbers == preferred_specialist).astype(jnp.int32)
            drawn_gate_scores = random_perturbation + 256 * popular_specialists + 2048 * remaining_headroom + preferred_increment
            score = drawn_gate_scores * EXPERTS + specialist_numbers
            score = jnp.where(counts < SPECIALIST_CAP, score, -1)
            node_grid = score.reshape(N_NODE, per_node)
            best = lax.top_k(node_grid, take)[0]
            usable = jnp.min(best, axis=1) >= 0
            node_score = jnp.where(usable, jnp.sum(best, axis=1), -1) * N_NODE + node_ids
            chosen = lax.top_k(node_score, NODE_PICK)[1].astype(jnp.int32)
            picked = lax.top_k(node_grid[chosen], take)[1].astype(jnp.int32) + chosen[:, None] * per_node
            picked = picked.reshape(TOP).astype(jnp.int32)
            counts = counts + jnp.sum((picked[:, None] == specialist_numbers[None, :]).astype(jnp.int32), axis=0)
            return (counts, picked)
        return lax.scan(step, jnp.zeros((EXPERTS,), jnp.int32), noise_block)[1]
    return jax.vmap(one_block)(noise).reshape(TOKENS, TOP).astype(jnp.int32)


def level_of(rng, shape, shards, low, largest):
    def one(position, shards_of):
        steps = jax.random.uniform(jax.random.fold_in(jax.random.fold_in(rng, 6), position), (shards_of,), jnp.float32, low / len(shards), largest / len(shards))
        return jnp.repeat(jnp.exp(steps), shape[position] // shards_of).reshape((-1,) + (1,) * (len(shape) - position - 1))

    level = one(*shards[0])
    for cut in shards[1:]:
        level = level * one(*cut)
    return level


def normal_values(stream_key, shape, scale, reach, pieces=(), held_as=jnp.bfloat16):
    loudness = level_of(stream_key, shape, pieces, -0.22, 0.18) if pieces else 1.0
    array = jax.random.normal(stream_key, shape, jnp.float32) * scale * loudness
    return jnp.minimum(jnp.maximum(array, -reach), reach).astype(held_as)


def setup_inputs(seed: int = 0) -> dict:
    seeds = jax.random.split(jax.random.key(seed), 6)
    return {
        "tokens": normal_values(seeds[0], (TOKENS, D), 1.0, 6.0, ((0, 32),)),
        "routes": draw_routes(jax.random.fold_in(seeds[5], 71), 0),
        "gates": jnp.clip(jnp.exp(math.log(0.5) - 2.306499 * jax.random.uniform(seeds[2], (TOKENS, TOP), jnp.float32) ** level_of(seeds[2], (TOKENS, TOP), ((0, 32),), -0.2, 0.2)), 0.049804688, 0.5).astype(jnp.bfloat16),
        "w_in": normal_values(seeds[3], (2 * EXPERTS, D // 2, 2 * H), D ** -0.5, 0.0625, ((0, 32),)),
        "w_out": normal_values(seeds[4], (2 * EXPERTS, H, D // 2), H ** -0.5, 0.1875, ((0, 32),)),
    }


def expert_rows(rows, w_first, w_second):
    width = w_second.shape[0]
    proj = jnp.dot(rows, w_first, preferred_element_type=jnp.float32)
    act = (jax.nn.silu(proj[:, :width]) * proj[:, width:]).astype(jnp.bfloat16)
    return jnp.dot(act, w_second, preferred_element_type=jnp.float32).astype(jnp.bfloat16)


def reference(tokens, routes, gates, w_in, w_out):
    picks = TOKENS * TOP
    flat_e = routes.reshape(picks).astype(jnp.int32)
    flat_t = (jnp.arange(picks, dtype=jnp.int32) // TOP).astype(jnp.int32)
    flat_g = gates.reshape(picks).astype(jnp.float32)
    counts = jnp.bincount(flat_e, length=EXPERTS).astype(jnp.int32)
    padded = ((counts + 127) // 128 * 128).astype(jnp.int32)
    pad_start = (jnp.cumsum(padded) - padded).astype(jnp.int32)
    live_start = (jnp.cumsum(counts) - counts).astype(jnp.int32)
    order = jnp.argsort(flat_e, stable=True).astype(jnp.int32)
    sorted_e = flat_e[order]
    rank_sorted = (jnp.arange(picks, dtype=jnp.int32) - live_start[sorted_e]).astype(jnp.int32)
    dest_sorted = (pad_start[sorted_e] + rank_sorted).astype(jnp.int32)
    dest = jnp.zeros((picks,), jnp.int32).at[order].set(dest_sorted)
    blocks = picks // 128 + EXPERTS
    slots = blocks * 128
    slot_token = jnp.full((slots,), TOKENS, jnp.int32).at[dest].set(flat_t)
    slot_gate = jnp.zeros((slots,), jnp.float32).at[dest].set(flat_g)
    slot_exp = jnp.zeros((slots,), jnp.int32).at[dest].set(flat_e)
    block_exp = jnp.max(slot_exp.reshape(blocks, 128), axis=1).astype(jnp.int32)

    def step(total, args):
        index_rows, expert, gate_rows = args
        start = (2 * expert).astype(jnp.int32)
        first = lax.dynamic_slice_in_dim(w_in, start, 2, 0).reshape(D, 2 * H)
        second_pair = lax.dynamic_slice_in_dim(w_out, start, 2, 0)
        second = jnp.concatenate([second_pair[0], second_pair[1]], axis=1)
        rows = jnp.take(tokens, index_rows, axis=0, mode="fill", fill_value=0)
        result = expert_rows(rows, first, second)
        total = total.at[index_rows].add(gate_rows[:, None] * result.astype(jnp.float32), mode="drop")
        return total, None

    start_total = jnp.zeros((TOKENS, D), jnp.float32)
    total, _ = lax.scan(step, start_total, (slot_token.reshape(blocks, 128), block_exp, slot_gate.reshape(blocks, 128)))
    return total.astype(jnp.bfloat16)
```

```python
import functools

import jax
import jax.numpy as jnp
from jax import lax
from jax.experimental import pallas as pl
from jax.experimental.pallas import tpu as pltpu

MESH = pl.DeviceIdType.MESH


def copy_to(src, dst, send_sem, recv_sem, device):
    return pltpu.make_async_remote_copy(
        src_ref=src,
        dst_ref=dst,
        send_sem=send_sem,
        recv_sem=recv_sem,
        device_id=device,
        device_id_type=MESH,
    )


def place():
    node = lax.axis_index("node")
    local = lax.axis_index("local")
    return node // 2, lax.rem(node, 2), local // 2, lax.rem(local, 2)


def device(y, c, z, x):
    return (y * 2 + c, z * 2 + x)


def greet(ny, m):
    y, c, z, x = place()
    barrier = pltpu.get_barrier_semaphore()

    def hello(dev):
        pl.semaphore_signal(barrier, inc=1, device_id=dev, device_id_type=MESH)

    hello(device(y, c, z, 1 - x))
    hello(device(y, 1 - c, z, x))
    for dy in range(1, ny):
        hello(device(lax.rem(y + dy, ny), c, z, x))

    @pl.when(z > 0)
    def _():
        hello(device(y, c, z - 1, x))

    @pl.when(z < m - 1)
    def _():
        hello(device(y, c, z + 1, x))

    ends = (z > 0).astype(jnp.int32) + (z < m - 1).astype(jnp.int32)
    pl.semaphore_wait(barrier, ny + 1 + ends)


def gather_kernel(q, ny, m, tok_ref, buf_ref, loc_sem, pair_sem, recv, zsend, ysend, csend):
    y, c, z, x = place()
    greet(ny, m)
    partner = device(y, c, z, 1 - x)

    def slab(yy, cc, zz):
        return buf_ref.at[yy, cc, zz]

    def arrived(yy, cc, zz):
        s = slab(yy, cc, zz)
        copy_to(s, s, pair_sem, recv.at[yy, cc, zz], partner).wait_recv()

    def up(zz):
        return copy_to(slab(y, c, zz), slab(y, c, zz), zsend.at[0, zz], recv.at[y, c, zz],
                       device(y, c, z + 1, x))

    def down(zz):
        return copy_to(slab(y, c, zz), slab(y, c, zz), zsend.at[1, zz], recv.at[y, c, zz],
                       device(y, c, z - 1, x))

    def across(dy, zz):
        return copy_to(slab(y, c, zz), slab(y, c, zz), ysend.at[dy, zz], recv.at[y, c, zz],
                       device(lax.rem(y + dy, ny), c, z, x))

    def core(yy, zz):
        return copy_to(slab(yy, c, zz), slab(yy, c, zz), csend.at[yy, zz], recv.at[yy, c, zz],
                       device(y, 1 - c, z, x))

    mine = pltpu.make_async_copy(tok_ref.at[q], slab(y, c, z), loc_sem)
    give = copy_to(tok_ref.at[1 - q], slab(y, c, z), pair_sem, recv.at[y, c, z], partner)

    @pl.when(x == q)
    def _():
        give.start()
        mine.start()
        mine.wait()

    @pl.when(x != q)
    def _():
        arrived(y, c, z)

    def have(zz, is_up, is_down):
        if is_up:
            @pl.when(z + 1 < m)
            def _():
                up(zz).start()
        if is_down:
            @pl.when(z > 0)
            def _():
                down(zz).start()
        for dy in range(1, ny):
            across(dy, zz).start()
        core(y, zz).start()

    def relay(zz):
        for dy in range(1, ny):
            yy = lax.rem(y + dy, ny)
            arrived(yy, c, zz)
            core(yy, zz).start()

    def both(s, act):
        if s == 0:
            act(z, True, True)
            return

        @pl.when(z - s >= 0)
        def _():
            act(z - s, True, False)

        @pl.when(z + s < m)
        def _():
            act(z + s, False, True)

    have(z, True, True)
    for s in range(1, m):
        def first(zz, is_up, is_down):
            arrived(y, c, zz)
            have(zz, is_up, is_down)

        both(s, first)
        both(s - 1, lambda zz, u, d: relay(zz))
    both(m - 1, lambda zz, u, d: relay(zz))

    @pl.when(x == q)
    def _():
        give.wait_send()

    for yy in range(ny):
        for zz in range(m):
            arrived(yy, 1 - c, zz)
            core(yy, zz).wait_send()
    for zz in range(m):
        for dy in range(1, ny):
            across(dy, zz).wait_send()

        @pl.when((z + 1 < m) & (z >= zz))
        def _():
            up(zz).wait_send()

        @pl.when((z > 0) & (z <= zz))
        def _():
            down(zz).wait_send()


def add_into(acc, other):
    rows = acc.shape[0]

    @pl.loop(0, rows // 16)
    def _(i):
        r = pl.ds(pl.multiple_of(i * 16, 16), 16)
        acc[r, :] = (acc[r, :].astype(jnp.float32) + other[r, :].astype(jnp.float32)).astype(
            acc.dtype
        )


def scatter_kernel(q, ny, m, in_ref, out_ref, own, got_c, got_y, got_z, load, csend, crecv,
                   ysend, yrecv, zsend, zrecv, psend, precv, osem):
    y, c, z, x = place()
    greet(ny, m)
    partner = device(y, c, z, 1 - x)

    def core(yy, zz):
        return copy_to(in_ref.at[yy, 1 - c, zz], got_c.at[yy, zz], csend.at[yy, zz],
                       crecv.at[yy, zz], device(y, 1 - c, z, x))

    def fetch(yy, zz):
        return pltpu.make_async_copy(in_ref.at[yy, c, zz], own.at[yy, zz], load.at[yy, zz])

    def across(dy, zz):
        return copy_to(own.at[lax.rem(y + dy, ny), zz], got_y.at[y, zz], ysend.at[dy, zz],
                       yrecv.at[y, zz], device(lax.rem(y + dy, ny), c, z, x))

    def up(zz):
        return copy_to(own.at[y, zz], got_z.at[0, zz], zsend.at[0, zz], zrecv.at[0, zz],
                       device(y, c, z + 1, x))

    def down(zz):
        return copy_to(own.at[y, zz], got_z.at[1, zz], zsend.at[1, zz], zrecv.at[1, zz],
                       device(y, c, z - 1, x))

    def far_first(act):
        for s in range(m - 1, 0, -1):
            @pl.when(z + s < m)
            def _():
                act(z + s, 1)

            @pl.when(z - s >= 0)
            def _():
                act(z - s, -1)
        act(z, 0)

    def start_cross(zz, way):
        for dy in range(1, ny):
            yy = lax.rem(y + dy, ny)
            core(yy, zz).start()
            fetch(yy, zz).start()

    def start_own(zz, way):
        core(y, zz).start()
        fetch(y, zz).start()

    far_first(start_cross)
    far_first(start_own)

    def chip_sum(yy, zz):
        fetch(yy, zz).wait()
        core(yy, zz).wait_recv()
        add_into(own.at[yy, zz], got_c.at[yy, zz])

    def send_cross(zz, way):
        for dy in range(1, ny):
            chip_sum(lax.rem(y + dy, ny), zz)
            across(dy, zz).start()

    far_first(send_cross)
    far_first(lambda zz, way: chip_sum(y, zz))

    def from_z(k, zz):
        copy_to(own.at[y, zz], got_z.at[k, zz], zsend.at[k, zz], zrecv.at[k, zz],
                partner).wait_recv()
        add_into(own.at[y, zz], got_z.at[k, zz])

    def line(zz, way):
        for dy in range(1, ny):
            yy = lax.rem(y + dy, ny)
            copy_to(own.at[y, zz], got_y.at[yy, zz], psend, yrecv.at[yy, zz], partner).wait_recv()
            add_into(own.at[y, zz], got_y.at[yy, zz])
        if way >= 0:
            @pl.when(z > 0)
            def _():
                from_z(0, zz)
        if way <= 0:
            @pl.when(z < m - 1)
            def _():
                from_z(1, zz)
        if way > 0:
            up(zz).start()
        if way < 0:
            down(zz).start()

    far_first(line)

    final = own.at[y, z]
    mine = pltpu.make_async_copy(final, out_ref.at[q], osem)
    give = copy_to(final, out_ref.at[1 - q], psend, precv, partner)

    @pl.when(x == q)
    def _():
        mine.start()
        mine.wait()
        give.wait_recv()

    @pl.when(x != q)
    def _():
        give.start()
        give.wait_send()

    for yy in range(ny):
        for zz in range(m):
            core(yy, zz).wait_send()
    for zz in range(m):
        for dy in range(1, ny):
            across(dy, zz).wait_send()

        @pl.when(z < zz)
        def _():
            up(zz).wait_send()

        @pl.when(z > zz)
        def _():
            down(zz).wait_send()


def gather_rows(q, ny, m, tok):
    _, rows, half = tok.shape
    sem = pltpu.SemaphoreType.DMA
    total = ny * 2 * m * rows * half * 2
    return pl.pallas_call(
        functools.partial(gather_kernel, q, ny, m),
        out_shape=jax.ShapeDtypeStruct((ny, 2, m, rows, half), tok.dtype),
        in_specs=[pl.BlockSpec(memory_space=pltpu.VMEM)],
        out_specs=pl.BlockSpec(memory_space=pl.ANY),
        scratch_shapes=[sem, sem, sem((ny, 2, m)), sem((2, m)), sem((ny, m)), sem((ny, m))],
        compiler_params=pltpu.CompilerParams(collective_id=q, has_side_effects=True),
        cost_estimate=pl.CostEstimate(flops=0, bytes_accessed=20 * total, transcendentals=0),
    )(tok)


def scatter_rows(q, ny, m, dense):
    rows, half = dense.shape[-2:]
    sem = pltpu.SemaphoreType.DMA
    vmem = pltpu.VMEM
    total = ny * 2 * m * rows * half * 2
    slab = (rows, half)
    return pl.pallas_call(
        functools.partial(scatter_kernel, q, ny, m),
        out_shape=jax.ShapeDtypeStruct((2, rows, half), dense.dtype),
        in_specs=[pl.BlockSpec(memory_space=pl.ANY)],
        out_specs=pl.BlockSpec(memory_space=pltpu.VMEM),
        scratch_shapes=[
            vmem((ny, m) + slab, dense.dtype),
            vmem((ny, m) + slab, dense.dtype),
            vmem((ny, m) + slab, dense.dtype),
            vmem((2, m) + slab, dense.dtype),
            sem((ny, m)),
            sem((ny, m)),
            sem((ny, m)),
            sem((ny, m)),
            sem((ny, m)),
            sem((2, m)),
            sem((2, m)),
            sem,
            sem,
            sem,
        ],
        compiler_params=pltpu.CompilerParams(
            collective_id=2 + q, has_side_effects=True, vmem_limit_bytes=62 * 1024 * 1024
        ),
        cost_estimate=pl.CostEstimate(flops=0, bytes_accessed=20 * total, transcendentals=0),
    )(dense)


def from_partner(block, axis):
    count = lax.axis_size(axis)
    return lax.ppermute(block, axis, [(i, i ^ 1) for i in range(count)])


def shards(tokens, routes, gates, w_in, w_out):
    rows, width = tokens.shape
    top = routes.shape[1]
    half = width // 2
    nodes = lax.axis_size("node")
    locals_ = lax.axis_size("local")
    ny, m = nodes // 2, locals_ // 2
    experts = nodes * m
    cap = 5 * rows * top // (4 * experts)
    w_first, w_second = w_in[0], w_out[0]
    hidden = w_second.shape[0]
    x = lax.rem(lax.axis_index("local"), 2)
    expert = (lax.axis_index("node") * locals_ + lax.axis_index("local")) // 2

    info = jnp.concatenate([routes.astype(jnp.bfloat16), gates], axis=1)
    info = lax.all_gather(info, ("node", "local"), axis=0, tiled=True)
    info = info.reshape(experts, 2, rows, 2 * top).astype(jnp.float32)
    named = info[..., :top] == expert.astype(jnp.float32)
    gate = jnp.sum(jnp.where(named, info[..., top:], 0.0), axis=3)
    chosen = jnp.any(named, axis=3)
    count = jnp.cumsum(chosen.astype(jnp.int32), axis=2) - 1
    slots = jnp.arange(cap, dtype=jnp.int32)
    match = chosen[:, :, None, :] & (count[:, :, None, :] == slots[None, None, :, None])
    placing = match.astype(jnp.bfloat16)
    weighting = jnp.where(match, gate[:, :, None, :], 0.0).astype(jnp.bfloat16)

    tok = tokens.reshape(rows, 2, half).transpose(1, 0, 2)
    parts = []
    for q in range(2):
        buf = gather_rows(q, ny, m, tok).reshape(experts, rows, half)
        picked = jnp.einsum(
            "bct,bth->bch", placing[:, q], buf, preferred_element_type=jnp.float32
        ).astype(jnp.bfloat16)
        part = jnp.dot(
            picked.reshape(experts * cap, half), w_first, preferred_element_type=jnp.float32
        ).astype(jnp.bfloat16)
        if q == 0:
            tok, part = lax.optimization_barrier((tok, part))
        parts.append((part, from_partner(part, "local")))
    outs = []
    for q in range(2):
        part, other = parts[q]
        proj = part.astype(jnp.float32) + other.astype(jnp.float32)
        act = (jax.nn.silu(proj[:, :hidden]) * proj[:, hidden:]).astype(jnp.bfloat16)
        result = jnp.dot(act, w_second, preferred_element_type=jnp.float32).astype(jnp.bfloat16)
        dense = jnp.einsum(
            "bct,bch->bth",
            weighting[:, q],
            result.reshape(experts, cap, half),
            preferred_element_type=jnp.float32,
        ).astype(jnp.bfloat16)
        outs.append(scatter_rows(q, ny, m, dense.reshape(ny, 2, m, rows, half)))
    final = jnp.where(x == 0, outs[0], outs[1])
    return final.transpose(1, 0, 2).reshape(rows, width)


def solution(mesh):
    spec = ("node", "local")
    return jax.shard_map(
        shards,
        mesh=mesh,
        in_specs=(
            P2(spec),
            P2(spec),
            P2(spec),
            P3(spec),
            P3(spec),
        ),
        out_specs=P2(spec),
        check_vma=False,
    )


def P2(spec):
    return jax.sharding.PartitionSpec(spec, None)


def P3(spec):
    return jax.sharding.PartitionSpec(spec, None, None)
```

```python
import functools

import jax
import jax.numpy as jnp
from jax import lax
from jax.experimental import pallas as pl
from jax.experimental.pallas import tpu as pltpu

MESH = pl.DeviceIdType.MESH


def copy_to(src, dst, send_sem, recv_sem, device):
    return pltpu.make_async_remote_copy(
        src_ref=src,
        dst_ref=dst,
        send_sem=send_sem,
        recv_sem=recv_sem,
        device_id=device,
        device_id_type=MESH,
    )


def place():
    node = lax.axis_index("node")
    local = lax.axis_index("local")
    return node // 2, lax.rem(node, 2), local // 2, lax.rem(local, 2)


def device(y, c, z, x):
    return (y * 2 + c, z * 2 + x)


def greet(ny, m, pair=True):
    y, c, z, x = place()
    barrier = pltpu.get_barrier_semaphore()

    def hello(dev):
        pl.semaphore_signal(barrier, inc=1, device_id=dev, device_id_type=MESH)

    if pair:
        hello(device(y, c, z, 1 - x))
    hello(device(y, 1 - c, z, x))
    for dy in range(1, ny):
        hello(device(lax.rem(y + dy, ny), c, z, x))

    @pl.when(z > 0)
    def _():
        hello(device(y, c, z - 1, x))

    @pl.when(z < m - 1)
    def _():
        hello(device(y, c, z + 1, x))

    ends = (z > 0).astype(jnp.int32) + (z < m - 1).astype(jnp.int32)
    pl.semaphore_wait(barrier, ny + int(pair) + ends)


def gather_kernel(q, ny, m, tok_ref, buf_ref, *rest):
    if q == 0:
        seed_ref, loc_sem, pair_sem, seed_sem, recv, zsend, ysend, csend = rest
    else:
        loc_sem, pair_sem, recv, zsend, ysend, csend = rest
    y, c, z, x = place()
    greet(ny, m, q == 0)
    partner = device(y, c, z, 1 - x)

    def slab(yy, cc, zz):
        return buf_ref.at[yy, cc, zz]

    def arrived(yy, cc, zz):
        s = slab(yy, cc, zz)
        copy_to(s, s, pair_sem, recv.at[yy, cc, zz], partner).wait_recv()

    def up(zz):
        return copy_to(slab(y, c, zz), slab(y, c, zz), zsend.at[0, zz], recv.at[y, c, zz],
                       device(y, c, z + 1, x))

    def down(zz):
        return copy_to(slab(y, c, zz), slab(y, c, zz), zsend.at[1, zz], recv.at[y, c, zz],
                       device(y, c, z - 1, x))

    def across(dy, zz):
        return copy_to(slab(y, c, zz), slab(y, c, zz), ysend.at[dy, zz], recv.at[y, c, zz],
                       device(lax.rem(y + dy, ny), c, z, x))

    def core(yy, zz):
        return copy_to(slab(yy, c, zz), slab(yy, c, zz), csend.at[yy, zz], recv.at[yy, c, zz],
                       device(y, 1 - c, z, x))

    if q == 0:
        mine = pltpu.make_async_copy(tok_ref.at[0], slab(y, c, z), loc_sem)
        give = copy_to(tok_ref.at[1], slab(y, c, z), pair_sem, recv.at[y, c, z], partner)
        keep_seed = pltpu.make_async_copy(tok_ref.at[1], seed_ref, loc_sem)
        give_seed = copy_to(tok_ref.at[0], seed_ref, pair_sem, seed_sem, partner)

        @pl.when(x == 0)
        def _():
            give.start()
            mine.start()
            mine.wait()

        @pl.when(x != 0)
        def _():
            give_seed.start()
            keep_seed.start()
            keep_seed.wait()
            arrived(y, c, z)
    else:
        mine = pltpu.make_async_copy(tok_ref, slab(y, c, z), loc_sem)
        mine.start()
        mine.wait()

    def have(zz, is_up, is_down):
        if is_up:
            @pl.when(z + 1 < m)
            def _():
                up(zz).start()
        if is_down:
            @pl.when(z > 0)
            def _():
                down(zz).start()
        for dy in range(1, ny):
            across(dy, zz).start()
        core(y, zz).start()

    def relay(zz):
        for dy in range(1, ny):
            yy = lax.rem(y + dy, ny)
            arrived(yy, c, zz)
            core(yy, zz).start()

    def both(s, act):
        if s == 0:
            act(z, True, True)
            return

        @pl.when(z - s >= 0)
        def _():
            act(z - s, True, False)

        @pl.when(z + s < m)
        def _():
            act(z + s, False, True)

    have(z, True, True)
    for s in range(1, m):
        def first(zz, is_up, is_down):
            arrived(y, c, zz)
            have(zz, is_up, is_down)

        both(s, first)
        both(s - 1, lambda zz, u, d: relay(zz))
    both(m - 1, lambda zz, u, d: relay(zz))

    if q == 0:
        @pl.when(x == 0)
        def _():
            give.wait_send()
            give_seed.wait_recv()

        @pl.when(x != 0)
        def _():
            give_seed.wait_send()

    for yy in range(ny):
        for zz in range(m):
            arrived(yy, 1 - c, zz)
            core(yy, zz).wait_send()
    for zz in range(m):
        for dy in range(1, ny):
            across(dy, zz).wait_send()

        @pl.when((z + 1 < m) & (z >= zz))
        def _():
            up(zz).wait_send()

        @pl.when((z > 0) & (z <= zz))
        def _():
            down(zz).wait_send()


def add_into(acc, other):
    rows = acc.shape[0]

    @pl.loop(0, rows // 16)
    def _(i):
        r = pl.ds(pl.multiple_of(i * 16, 16), 16)
        acc[r, :] = (acc[r, :].astype(jnp.float32) + other[r, :].astype(jnp.float32)).astype(
            acc.dtype
        )


def scatter_kernel(q, ny, m, in_ref, out_ref, own, got_c, got_y, got_z, load, csend, crecv,
                   ysend, yrecv, zsend, zrecv, psend, precv, osem):
    y, c, z, x = place()
    greet(ny, m)
    partner = device(y, c, z, 1 - x)

    def core(yy, zz):
        return copy_to(in_ref.at[yy, 1 - c, zz], got_c.at[yy, zz], csend.at[yy, zz],
                       crecv.at[yy, zz], device(y, 1 - c, z, x))

    def fetch(yy, zz):
        return pltpu.make_async_copy(in_ref.at[yy, c, zz], own.at[yy, zz], load.at[yy, zz])

    def across(dy, zz):
        return copy_to(own.at[lax.rem(y + dy, ny), zz], got_y.at[y, zz], ysend.at[dy, zz],
                       yrecv.at[y, zz], device(lax.rem(y + dy, ny), c, z, x))

    def up(zz):
        return copy_to(own.at[y, zz], got_z.at[0, zz], zsend.at[0, zz], zrecv.at[0, zz],
                       device(y, c, z + 1, x))

    def down(zz):
        return copy_to(own.at[y, zz], got_z.at[1, zz], zsend.at[1, zz], zrecv.at[1, zz],
                       device(y, c, z - 1, x))

    def far_first(act):
        for s in range(m - 1, 0, -1):
            @pl.when(z + s < m)
            def _():
                act(z + s, 1)

            @pl.when(z - s >= 0)
            def _():
                act(z - s, -1)
        act(z, 0)

    def start_cross(zz, way):
        for dy in range(1, ny):
            yy = lax.rem(y + dy, ny)
            core(yy, zz).start()
            fetch(yy, zz).start()

    def start_own(zz, way):
        core(y, zz).start()
        fetch(y, zz).start()

    far_first(start_cross)
    far_first(start_own)

    def chip_sum(yy, zz):
        fetch(yy, zz).wait()
        core(yy, zz).wait_recv()
        add_into(own.at[yy, zz], got_c.at[yy, zz])

    def send_cross(zz, way):
        for dy in range(1, ny):
            chip_sum(lax.rem(y + dy, ny), zz)
            across(dy, zz).start()

    far_first(send_cross)
    far_first(lambda zz, way: chip_sum(y, zz))

    def from_z(k, zz):
        copy_to(own.at[y, zz], got_z.at[k, zz], zsend.at[k, zz], zrecv.at[k, zz],
                partner).wait_recv()
        add_into(own.at[y, zz], got_z.at[k, zz])

    def line(zz, way):
        for dy in range(1, ny):
            yy = lax.rem(y + dy, ny)
            copy_to(own.at[y, zz], got_y.at[yy, zz], psend, yrecv.at[yy, zz], partner).wait_recv()
            add_into(own.at[y, zz], got_y.at[yy, zz])
        if way >= 0:
            @pl.when(z > 0)
            def _():
                from_z(0, zz)
        if way <= 0:
            @pl.when(z < m - 1)
            def _():
                from_z(1, zz)
        if way > 0:
            up(zz).start()
        if way < 0:
            down(zz).start()

    far_first(line)

    final = own.at[y, z]
    mine = pltpu.make_async_copy(final, out_ref.at[q], osem)
    give = copy_to(final, out_ref.at[1 - q], psend, precv, partner)

    @pl.when(x == q)
    def _():
        mine.start()
        mine.wait()
        give.wait_recv()

    @pl.when(x != q)
    def _():
        give.start()
        give.wait_send()

    for yy in range(ny):
        for zz in range(m):
            core(yy, zz).wait_send()
    for zz in range(m):
        for dy in range(1, ny):
            across(dy, zz).wait_send()

        @pl.when(z < zz)
        def _():
            up(zz).wait_send()

        @pl.when(z > zz)
        def _():
            down(zz).wait_send()


def gather_rows(q, ny, m, tok):
    rows, width = tok.shape[-2:]
    sem = pltpu.SemaphoreType.DMA
    total = ny * 2 * m * rows * width * 2
    shape = jax.ShapeDtypeStruct((ny, 2, m, rows, width), tok.dtype)
    anywhere = pl.BlockSpec(memory_space=pl.ANY)
    vmem = pl.BlockSpec(memory_space=pltpu.VMEM)
    seed = jax.ShapeDtypeStruct((rows, width), tok.dtype)
    sems = [sem, sem] + [sem] * (q == 0)
    return pl.pallas_call(
        functools.partial(gather_kernel, q, ny, m),
        out_shape=(shape, seed) if q == 0 else shape,
        in_specs=[vmem],
        out_specs=(anywhere, vmem) if q == 0 else anywhere,
        scratch_shapes=sems + [sem((ny, 2, m)), sem((2, m)), sem((ny, m)), sem((ny, m))],
        compiler_params=pltpu.CompilerParams(collective_id=q, has_side_effects=True),
        cost_estimate=pl.CostEstimate(flops=0, bytes_accessed=20 * total, transcendentals=0),
    )(tok)


def scatter_rows(q, ny, m, dense):
    rows, half = dense.shape[-2:]
    sem = pltpu.SemaphoreType.DMA
    vmem = pltpu.VMEM
    total = ny * 2 * m * rows * half * 2
    slab = (rows, half)
    return pl.pallas_call(
        functools.partial(scatter_kernel, q, ny, m),
        out_shape=jax.ShapeDtypeStruct((2, rows, half), dense.dtype),
        in_specs=[pl.BlockSpec(memory_space=pl.ANY)],
        out_specs=pl.BlockSpec(memory_space=pltpu.VMEM),
        scratch_shapes=[
            vmem((ny, m) + slab, dense.dtype),
            vmem((ny, m) + slab, dense.dtype),
            vmem((ny, m) + slab, dense.dtype),
            vmem((2, m) + slab, dense.dtype),
            sem((ny, m)),
            sem((ny, m)),
            sem((ny, m)),
            sem((ny, m)),
            sem((ny, m)),
            sem((2, m)),
            sem((2, m)),
            sem,
            sem,
            sem,
        ],
        compiler_params=pltpu.CompilerParams(
            collective_id=2 + q, has_side_effects=True, vmem_limit_bytes=62 * 1024 * 1024
        ),
        cost_estimate=pl.CostEstimate(flops=0, bytes_accessed=20 * total, transcendentals=0),
    )(dense)


def from_partner(block, axis):
    count = lax.axis_size(axis)
    return lax.ppermute(block, axis, [(i, i ^ 1) for i in range(count)])


def shards(tokens, routes, gates, w_in, w_out):
    rows, width = tokens.shape
    top = routes.shape[1]
    half = width // 2
    nodes = lax.axis_size("node")
    locals_ = lax.axis_size("local")
    ny, m = nodes // 2, locals_ // 2
    experts = nodes * m
    cap = 5 * rows * top // (4 * experts)
    w_first, w_second = w_in[0], w_out[0]
    hidden = w_second.shape[0]
    x = lax.rem(lax.axis_index("local"), 2)
    expert = (lax.axis_index("node") * locals_ + lax.axis_index("local")) // 2

    lanes = 128 * ((2 * top + 127) // 128)
    info = jnp.concatenate([routes.astype(jnp.bfloat16), gates], axis=1)
    info = jnp.pad(info, ((0, 0), (0, lanes - 2 * top)))
    tok = jnp.stack(
        [jnp.concatenate([tokens[:, h * half : (h + 1) * half], info], axis=1) for h in range(2)]
    )
    slots = jnp.arange(cap, dtype=jnp.int32)
    parts, weights = [], []
    for q in range(2):
        if q == 0:
            buf, seed = gather_rows(q, ny, m, tok)
        else:
            buf = gather_rows(q, ny, m, seed)
        buf = buf.reshape(experts, rows, half + lanes)
        info = buf[..., half : half + 2 * top].astype(jnp.float32)
        named = info[..., :top] == expert.astype(jnp.float32)
        gate = jnp.sum(jnp.where(named, info[..., top:], 0.0), axis=2)
        chosen = jnp.any(named, axis=2)
        count = jnp.cumsum(chosen.astype(jnp.int32), axis=1) - 1
        match = chosen[:, None, :] & (count[:, None, :] == slots[None, :, None])
        weights.append(jnp.where(match, gate[:, None, :], 0.0).astype(jnp.bfloat16))
        picked = jnp.einsum(
            "bct,bth->bch",
            match.astype(jnp.bfloat16),
            buf[..., :half],
            preferred_element_type=jnp.float32,
        ).astype(jnp.bfloat16)
        part = jnp.dot(
            picked.reshape(experts * cap, half), w_first, preferred_element_type=jnp.float32
        ).astype(jnp.bfloat16)
        if q == 0:
            seed, part = lax.optimization_barrier((seed, part))
        parts.append((part, from_partner(part, "local")))
    outs = []
    for q in range(2):
        part, other = parts[q]
        proj = part.astype(jnp.float32) + other.astype(jnp.float32)
        act = (jax.nn.silu(proj[:, :hidden]) * proj[:, hidden:]).astype(jnp.bfloat16)
        result = jnp.dot(act, w_second, preferred_element_type=jnp.float32).astype(jnp.bfloat16)
        dense = jnp.einsum(
            "bct,bch->bth",
            weights[q],
            result.reshape(experts, cap, half),
            preferred_element_type=jnp.float32,
        ).astype(jnp.bfloat16)
        outs.append(scatter_rows(q, ny, m, dense.reshape(ny, 2, m, rows, half)))
    final = jnp.where(x == 0, outs[0], outs[1])
    return final.transpose(1, 0, 2).reshape(rows, width)


def solution(mesh):
    spec = ("node", "local")
    return jax.shard_map(
        shards,
        mesh=mesh,
        in_specs=(
            P2(spec),
            P2(spec),
            P2(spec),
            P3(spec),
            P3(spec),
        ),
        out_specs=P2(spec),
        check_vma=False,
    )


def P2(spec):
    return jax.sharding.PartitionSpec(spec, None)


def P3(spec):
    return jax.sharding.PartitionSpec(spec, None, None)
```
